32 devices in a mesh: row: 4 (over y, core), col: 8 (over z, x).
Axes of the slice: x: 2, y: 2, z: 4, core: 2. Of those that a mesh axis runs over, the one named last changes fastest.
Arguments:
- tokens: bfloat16 [64, 16384], P('row', 'col'), may hold values from -6 to 6
- gate_weight: bfloat16 [16384, 26624], P('col', 'row'), may hold values from -0.046875 to 0.046875
- up_weight: bfloat16 [16384, 26624], P('col', 'row'), may hold values from -0.046875 to 0.046875
Outputs:
- hidden: bfloat16 [64, 26624], P(None, 'row')
The draws below stay inside these ranges and needn't reach their ends.
All inputs are finite; a program needn't handle non-finite values.
Results may differ from the reference program's by a relative error of at most 0.001.
Values may be sent and summed in bfloat16 or wider, within the bound.
A program may use at most 128 MiB of HBM per device.

```python
import jax
import jax.numpy as jnp
from jax import lax

D = 16384
FF = 26624
TOKENS = 64
N_COL = 8


def strengthened(result, rng, source, target, parts, factor):
    owner, partner = [(jnp.arange(result.shape[axis_at]) // (result.shape[axis_at] // parts)).reshape([-1 if axis == axis_at else 1 for axis in range(result.ndim)]) for axis_at in (source, target)]
    chosen = jax.random.permutation(rng, parts)[partner]
    strong = (owner == chosen) | (owner == (partner + parts // 2) % parts)
    return jnp.where(strong, factor * result, result)


def level_of(key, extent, shards, least, largest):
    gain, own = 1.0, jax.random.fold_in(key, 6)
    for dim, blocks in shards:
        heights = jnp.exp(jax.random.uniform(jax.random.fold_in(own, dim), (blocks,), jnp.float32, least / len(shards), largest / len(shards)))
        gain = gain * jnp.repeat(heights, extent[dim] // blocks).reshape([-1 if axis == dim else 1 for axis in range(len(extent))])
    return gain


def noise(key, shape, width, limit, pieces=(), held_as=jnp.bfloat16):
    loudness = level_of(key, shape, pieces, -0.22, 0.18) if pieces else 1.0
    drawn = jax.random.normal(key, shape, jnp.float32) * width * loudness
    return jnp.minimum(jnp.maximum(drawn, -limit), limit).astype(held_as)


def heavy_noise(key, extent, scale, reach, split, heavy, kind=jnp.bfloat16):
    entries = scale * jax.random.normal(key, extent, jnp.float32)
    if split:
        entries = entries * level_of(key, extent, split, -0.22, 0.18)
    return jnp.clip(strengthened(entries, jax.random.fold_in(key, 3), *heavy), -reach, reach).astype(kind)


def setup_inputs(seed: int = 0) -> dict:
    arg_keys = jax.random.split(jax.random.key(seed), 4)
    return {
        "tokens": heavy_noise(arg_keys[0], (TOKENS, D), 1.0, 6.0, ((0, 4), (1, 8)), (1, 0, 8, 2.0)),
        "gate_weight": noise(arg_keys[1], (D, FF), D ** -0.5, 0.046875, ((0, 8), (1, 4))),
        "up_weight": noise(arg_keys[2], (D, FF), D ** -0.5, 0.046875, ((0, 8), (1, 4))),
    }


def reference(tokens, gate_weight, up_weight):
    stride = D // N_COL

    def accumulate(totals, index):
        offset = (index * stride).astype(jnp.int32)
        feature_cols = lax.dynamic_slice_in_dim(tokens, offset, stride, 1)
        gate_block = lax.dynamic_slice_in_dim(gate_weight, offset, stride, 0)
        up_block = lax.dynamic_slice_in_dim(up_weight, offset, stride, 0)
        gate_part = jnp.dot(feature_cols, gate_block, preferred_element_type=jnp.float32)
        up_part = jnp.dot(feature_cols, up_block, preferred_element_type=jnp.float32)
        return (totals[0] + gate_part, totals[1] + up_part), None

    zeros = jnp.zeros((TOKENS, FF), jnp.float32)
    (gate, up), _ = lax.scan(accumulate, (zeros, zeros), jnp.arange(N_COL, dtype=jnp.int32))
    return (jax.nn.silu(gate) * up).astype(jnp.bfloat16)
```

```python
import functools

import jax
import jax.numpy as jnp
from jax import lax
from jax.experimental import pallas as pl
from jax.experimental.pallas import tpu as pltpu
from jax.sharding import PartitionSpec as P

MESH = pl.DeviceIdType.MESH

BUFFERS = 4
LAG = 2
WIDEST = 512
GATHER_REVERSED = True


def digits_of(n):
    bits = n.bit_length() - 1
    out = [(1, 2)]
    weight = 2
    if SPLIT_Z:
        for _ in range(bits - 1):
            out.append((weight, 2))
            weight *= 2
    elif bits > 1:
        out.append((2, n // 2))
    return out


SPLIT_Z = True


LANES = 128
SPAN, FLOOR = 175.0, -87.0


def across(tile, width):
    return jnp.concatenate([tile] * (width // LANES), axis=1)


def encode(x, inverse):
    size = jnp.exp(jnp.abs(x) * across(inverse * SPAN, x.shape[1]) + FLOOR)
    return jnp.where(x < 0, -size, size).astype(jnp.bfloat16)


def decode(y, peak):
    y = y.astype(jnp.float32)
    size = (jnp.log(jnp.abs(y)) - FLOOR) * across(peak * (1.0 / SPAN), y.shape[1])
    return jnp.where(y < 0, -size, size)


def kernel(n_row, n_col, chunks, width, tok_hbm, gate_hbm, up_hbm, out_hbm, *scratch):
    digits = digits_of(n_col)
    stages = len(digits)
    xg, wbuf, acc = scratch[0:3]
    held = scratch[3 : 3 + stages - 1]
    scratch = scratch[2 + stages :]
    sends, recvs, (gath, ) = scratch[:stages], scratch[stages : 2 * stages], scratch[2 * stages : 2 * stages + 1]
    tok_sem, tok_send, tok_recv, w_sem, out_sem = scratch[2 * stages + 1 : 2 * stages + 6]
    rs_send = scratch[2 * stages + 6 : 3 * stages + 6]
    rs_recv = scratch[3 * stages + 6 : 4 * stages + 6]
    ag_send = scratch[4 * stages + 6 : 5 * stages + 6]
    ag_recv = scratch[5 * stages + 6 : 6 * stages + 6]

    row, col = lax.axis_index("row"), lax.axis_index("col")
    mine = [(col // weight) % radix for weight, radix in digits]

    def peer(stage, offset):
        weight, radix = digits[stage]
        return col + ((mine[stage] + offset) % radix - mine[stage]) * weight

    def weights(c, slot):
        cols = pl.ds(pl.multiple_of(c * width, width), width)
        return [
            pltpu.make_async_copy(hbm.at[:, cols], wbuf.at[slot, k], w_sem.at[slot, k])
            for k, hbm in enumerate((gate_hbm, up_hbm))
        ]

    own = pltpu.make_async_copy(tok_hbm, xg.at[row], tok_sem)
    own.start()
    for c in range(min(BUFFERS, chunks)):
        for copy in weights(c, c):
            copy.start()

    barrier = pltpu.get_barrier_semaphore()
    greeted = 0
    for o in range(1, n_row):
        pl.semaphore_signal(barrier, inc=1, device_id=((row + o) % n_row, col), device_id_type=MESH)
        greeted += 1
    for i, (_, radix) in enumerate(digits):
        for o in range(1, radix):
            pl.semaphore_signal(barrier, inc=1, device_id=(row, peer(i, o)), device_id_type=MESH)
            greeted += 1
    pl.semaphore_wait(barrier, greeted)
    own.wait()

    def token_copy(o, place):
        return pltpu.make_async_remote_copy(
            src_ref=xg.at[place], dst_ref=xg.at[place], send_sem=tok_send.at[o - 1], recv_sem=tok_recv.at[o - 1],
            device_id=((row + o) % n_row, col), device_id_type=MESH)

    for o in range(1, n_row):
        token_copy(o, row).start()
    for o in range(1, n_row):
        token_copy(o, (row + n_row - o) % n_row).wait_recv()
    for o in range(1, n_row):
        token_copy(o, row).wait_send()

    def rs_copy(i, o, c):
        return pltpu.make_async_remote_copy(
            src_ref=sends[i].at[c, o - 1], dst_ref=recvs[i].at[c, o - 1],
            send_sem=rs_send[i].at[o - 1, c], recv_sem=rs_recv[i].at[o - 1, c],
            device_id=(row, peer(i, o)), device_id_type=MESH)

    def send_parts(i, source, c):
        sub = source.shape[1] // digits[i][1]
        for o in range(1, digits[i][1]):
            to = (mine[i] + o) % digits[i][1]
            for k in range(2):
                parts = [source[c, to * sub + g, k] for g in range(sub)]
                peak = functools.reduce(jnp.maximum, [
                    jnp.abs(part[:, at : at + LANES]) for part in parts for at in range(0, width, LANES)])
                peak = jnp.maximum(peak * 1.01, 1e-37).astype(jnp.bfloat16)
                sends[i][c, o - 1, k, :, sub * width :] = peak
                inverse = 1.0 / peak.astype(jnp.float32)
                for g, part in enumerate(parts):
                    sends[i][c, o - 1, k, :, g * width : (g + 1) * width] = encode(part, inverse)
            rs_copy(i, o, c).start()

    def summed(i, source, c, sink):
        sub = source.shape[1] // digits[i][1]
        for o in range(1, digits[i][1]):
            rs_copy(i, o, c).wait_recv()
        for k in range(2):
            peaks = [recvs[i][c, o, k, :, sub * width :].astype(jnp.float32) for o in range(digits[i][1] - 1)]
            for g in range(sub):
                total = source[c, mine[i] * sub + g, k]
                for o, peak in enumerate(peaks):
                    total = total + decode(recvs[i][c, o, k, :, g * width : (g + 1) * width], peak)
                sink(g, k, total)

    order = list(range(stages))[::-1] if GATHER_REVERSED else list(range(stages))

    def gathered_place(a, c, shift):
        index = [c]
        for i in range(stages):
            if i in order[:a]:
                index.append(slice(None))
            elif i == order[a]:
                index.append((mine[i] + digits[i][1] + shift) % digits[i][1])
            else:
                index.append(mine[i])
        return gath.at[tuple(index)]

    def ag_copy(a, o, c, shift):
        ref = gathered_place(a, c, shift)
        return pltpu.make_async_remote_copy(
            src_ref=ref, dst_ref=ref, send_sem=ag_send[a].at[o - 1, c], recv_sem=ag_recv[a].at[o - 1, c],
            device_id=(row, peer(order[a], o)), device_id_type=MESH)

    def ag_start(a, c):
        for o in range(1, digits[order[a]][1]):
            ag_copy(a, o, c, 0).start()

    def ag_wait(a, c):
        for o in range(1, digits[order[a]][1]):
            ag_copy(a, o, c, -o).wait_recv()

    def out_copy(c):
        cols = pl.ds(pl.multiple_of(c * width, width), width)
        return pltpu.make_async_copy(gath.at[c], out_hbm.at[(slice(None),) * (stages + 1) + (cols,)], out_sem.at[c])

    def multiply(c):
        slot = c % BUFFERS
        for k, copy in enumerate(weights(c, slot)):
            copy.wait()
            x = xg[...].reshape(-1, xg.shape[-1])
            part = jnp.dot(x, wbuf[slot, k], preferred_element_type=jnp.float32)
            acc[c, :, k] = part.reshape(n_col, -1, width)
        send_parts(0, acc, c)

        @pl.when(c + BUFFERS < chunks)
        def _():
            for copy in weights(c + BUFFERS, slot):
                copy.start()

    def reduce_step(i, c):
        source = acc if i == 0 else held[i - 1]
        if i < stages - 1:
            def keep(g, k, total):
                held[i][c, g, k] = total

            summed(i, source, c, keep)
            send_parts(i + 1, held[i], c)
        else:
            sums = []
            summed(i, source, c, lambda g, k, total: sums.append(total))
            gate, up = sums
            gath[(c, *mine)] = (gate / (1.0 + jnp.exp(-gate)) * up).astype(jnp.bfloat16)
            ag_start(0, c)

    def gather_step(a, c):
        ag_wait(a, c)
        if a < stages - 1:
            ag_start(a + 1, c)
        else:
            out_copy(c).start()

    steps = [multiply]
    steps += [functools.partial(reduce_step, i) for i in range(stages)]
    steps += [functools.partial(gather_step, a) for a in range(stages)]

    def turn(t, carry):
        for s, step in enumerate(steps):
            c = t - s * LAG

            @pl.when(jnp.logical_and(c >= 0, c < chunks))
            def _(c=c, step=step):
                step(c)

        return carry

    lax.fori_loop(0, chunks + (len(steps) - 1) * LAG, turn, 0)

    def drain(c, carry):
        for i in range(stages):
            for o in range(1, digits[i][1]):
                rs_copy(i, o, c).wait_send()
        for a in range(stages):
            for o in range(1, digits[order[a]][1]):
                ag_copy(a, o, c, 0).wait_send()
        out_copy(c).wait()
        return carry

    lax.fori_loop(0, chunks, drain, 0)


def solution(mesh):
    n_row, n_col = mesh.shape["row"], mesh.shape["col"]

    def local(tokens, gate_weight, up_weight):
        own_tokens, depth = tokens.shape
        columns = gate_weight.shape[1]
        each = own_tokens * n_row // n_col
        width = max(w for w in range(128, WIDEST + 1, 128) if columns % w == 0)
        chunks = columns // width
        digits = digits_of(n_col)
        radices = tuple(radix for _, radix in digits)
        subs, count = [], n_col
        for radix in radices:
            count //= radix
            subs.append(count)
        parts = [(chunks, radix - 1, 2, each, sub * width + LANES) for radix, sub in zip(radices, subs)]
        scratch = [
            pltpu.VMEM((n_row, own_tokens, depth), jnp.bfloat16),
            pltpu.VMEM((BUFFERS, 2, depth, width), jnp.bfloat16),
            pltpu.VMEM((chunks, n_col, 2, each, width), jnp.float32),
        ]
        scratch += [pltpu.VMEM((chunks, sub, 2, each, width), jnp.float32) for sub in subs[:-1]]
        scratch += [pltpu.VMEM(shape, jnp.bfloat16) for shape in parts]
        scratch += [pltpu.VMEM(shape, jnp.bfloat16) for shape in parts]
        scratch += [pltpu.VMEM((chunks, *radices, each, width), jnp.bfloat16)]
        dma = pltpu.SemaphoreType.DMA
        scratch += [dma, dma((n_row - 1,)), dma((n_row - 1,)), dma((BUFFERS, 2)), dma((chunks,))]
        for _ in range(2):
            scratch += [dma((radix - 1, chunks)) for radix in radices]
        ordered = radices[::-1] if GATHER_REVERSED else radices
        for _ in range(2):
            scratch += [dma((radix - 1, chunks)) for radix in ordered]
        out = pl.pallas_call(
            functools.partial(kernel, n_row, n_col, chunks, width),
            out_shape=jax.ShapeDtypeStruct((*radices, each, columns), jnp.bfloat16),
            in_specs=[pl.BlockSpec(memory_space=pl.ANY)] * 3,
            out_specs=pl.BlockSpec(memory_space=pl.ANY),
            scratch_shapes=scratch,
            compiler_params=pltpu.CompilerParams(
                collective_id=0, has_side_effects=True, vmem_limit_bytes=60 * 2**20),
        )(tokens, gate_weight, up_weight)
        return out.reshape(n_col * each, columns)

    in_specs = (P("row", "col"), P("col", "row"), P("col", "row"))
    return jax.shard_map(local, mesh=mesh, in_specs=in_specs, out_specs=P(None, "row"), check_vma=False)
```

```python
import functools

import jax
import jax.numpy as jnp
from jax import lax
from jax.experimental import pallas as pl
from jax.experimental.pallas import tpu as pltpu
from jax.sharding import PartitionSpec as P

MESH = pl.DeviceIdType.MESH

BUFFERS = 4
LAG = 3
WIDEST = 512
GATHER_REVERSED = True


def digits_of(n):
    bits = n.bit_length() - 1
    out = [(1, 2)]
    weight = 2
    if SPLIT_Z:
        for _ in range(bits - 1):
            out.append((weight, 2))
            weight *= 2
    elif bits > 1:
        out.append((2, n // 2))
    return out


SPLIT_Z = True


LANES = 128
SPAN, FLOOR = 175.0, -87.0


def across(tile, width):
    return jnp.concatenate([tile] * (width // LANES), axis=1)


def encode(x, inverse):
    size = jnp.exp(jnp.abs(x) * across(inverse * SPAN, x.shape[1]) + FLOOR)
    return jnp.where(x < 0, -size, size).astype(jnp.bfloat16)


def decode(y, peak):
    y = y.astype(jnp.float32)
    size = (jnp.log(jnp.abs(y)) - FLOOR) * across(peak * (1.0 / SPAN), y.shape[1])
    return jnp.where(y < 0, -size, size)


def kernel(n_row, n_col, chunks, width, tok_hbm, gate_hbm, up_hbm, out_hbm, *scratch):
    digits = digits_of(n_col)
    stages = len(digits)
    xg, wbuf, acc = scratch[0:3]
    held = scratch[3 : 3 + stages - 1]
    scratch = scratch[2 + stages :]
    sends, recvs, (gath, ) = scratch[:stages], scratch[stages : 2 * stages], scratch[2 * stages : 2 * stages + 1]
    tok_sem, tok_send, tok_recv, w_sem, out_sem = scratch[2 * stages + 1 : 2 * stages + 6]
    rs_send = scratch[2 * stages + 6 : 3 * stages + 6]
    rs_recv = scratch[3 * stages + 6 : 4 * stages + 6]
    ag_send = scratch[4 * stages + 6 : 5 * stages + 6]
    ag_recv = scratch[5 * stages + 6 : 6 * stages + 6]

    row, col = lax.axis_index("row"), lax.axis_index("col")
    mine = [(col // weight) % radix for weight, radix in digits]

    def peer(stage, offset):
        weight, radix = digits[stage]
        return col + ((mine[stage] + offset) % radix - mine[stage]) * weight

    def weights(c, slot):
        cols = pl.ds(pl.multiple_of(c * width, width), width)
        return [
            pltpu.make_async_copy(hbm.at[:, cols], wbuf.at[slot, k], w_sem.at[slot, k])
            for k, hbm in enumerate((gate_hbm, up_hbm))
        ]

    own = pltpu.make_async_copy(tok_hbm, xg.at[row], tok_sem)
    own.start()
    for c in range(min(BUFFERS, chunks)):
        for copy in weights(c, c):
            copy.start()

    barrier = pltpu.get_barrier_semaphore()
    greeted = 0
    for o in range(1, n_row):
        pl.semaphore_signal(barrier, inc=1, device_id=((row + o) % n_row, col), device_id_type=MESH)
        greeted += 1
    for i, (_, radix) in enumerate(digits):
        for o in range(1, radix):
            pl.semaphore_signal(barrier, inc=1, device_id=(row, peer(i, o)), device_id_type=MESH)
            greeted += 1
    pl.semaphore_wait(barrier, greeted)
    own.wait()

    def token_copy(o, place):
        return pltpu.make_async_remote_copy(
            src_ref=xg.at[place], dst_ref=xg.at[place], send_sem=tok_send.at[o - 1], recv_sem=tok_recv.at[o - 1],
            device_id=((row + o) % n_row, col), device_id_type=MESH)

    for o in range(1, n_row):
        token_copy(o, row).start()
    for o in range(1, n_row):
        token_copy(o, (row + n_row - o) % n_row).wait_recv()
    for o in range(1, n_row):
        token_copy(o, row).wait_send()

    def rs_copy(i, o, c):
        return pltpu.make_async_remote_copy(
            src_ref=sends[i].at[c, o - 1], dst_ref=recvs[i].at[c, o - 1],
            send_sem=rs_send[i].at[o - 1, c], recv_sem=rs_recv[i].at[o - 1, c],
            device_id=(row, peer(i, o)), device_id_type=MESH)

    def send_parts(i, source, c):
        sub = source.shape[1] // digits[i][1]
        for o in range(1, digits[i][1]):
            to = (mine[i] + o) % digits[i][1]
            for k in range(2):
                parts = [source[c, to * sub + g, k] for g in range(sub)]
                peak = functools.reduce(jnp.maximum, [
                    jnp.abs(part[:, at : at + LANES]) for part in parts for at in range(0, width, LANES)])
                peak = jnp.maximum(peak * 1.01, 1e-37).astype(jnp.bfloat16)
                sends[i][c, o - 1, k, :, sub * width :] = peak
                inverse = 1.0 / peak.astype(jnp.float32)
                for g, part in enumerate(parts):
                    sends[i][c, o - 1, k, :, g * width : (g + 1) * width] = encode(part, inverse)
            rs_copy(i, o, c).start()

    def summed(i, source, c, sink):
        sub = source.shape[1] // digits[i][1]
        for o in range(1, digits[i][1]):
            rs_copy(i, o, c).wait_recv()
        for k in range(2):
            peaks = [recvs[i][c, o, k, :, sub * width :].astype(jnp.float32) for o in range(digits[i][1] - 1)]
            for g in range(sub):
                total = source[c, mine[i] * sub + g, k]
                for o, peak in enumerate(peaks):
                    total = total + decode(recvs[i][c, o, k, :, g * width : (g + 1) * width], peak)
                sink(g, k, total)

    order = list(range(stages))[::-1] if GATHER_REVERSED else list(range(stages))

    def gathered_place(a, c, shift):
        index = [c]
        for i in range(stages):
            if i in order[:a]:
                index.append(slice(None))
            elif i == order[a]:
                index.append((mine[i] + digits[i][1] + shift) % digits[i][1])
            else:
                index.append(mine[i])
        return gath.at[tuple(index)]

    def ag_copy(a, o, c, shift):
        ref = gathered_place(a, c, shift)
        return pltpu.make_async_remote_copy(
            src_ref=ref, dst_ref=ref, send_sem=ag_send[a].at[o - 1, c], recv_sem=ag_recv[a].at[o - 1, c],
            device_id=(row, peer(order[a], o)), device_id_type=MESH)

    def ag_start(a, c):
        for o in range(1, digits[order[a]][1]):
            ag_copy(a, o, c, 0).start()

    def ag_wait(a, c):
        for o in range(1, digits[order[a]][1]):
            ag_copy(a, o, c, -o).wait_recv()

    def out_copy(c):
        cols = pl.ds(pl.multiple_of(c * width, width), width)
        return pltpu.make_async_copy(gath.at[c], out_hbm.at[(slice(None),) * (stages + 1) + (cols,)], out_sem.at[c])

    def multiply(c):
        slot = c % BUFFERS
        for k, copy in enumerate(weights(c, slot)):
            copy.wait()
            x = xg[...].reshape(-1, xg.shape[-1])
            part = jnp.dot(x, wbuf[slot, k], preferred_element_type=jnp.float32)
            acc[c, :, k] = part.reshape(n_col, -1, width)
        send_parts(0, acc, c)

        @pl.when(c + BUFFERS < chunks)
        def _():
            for copy in weights(c + BUFFERS, slot):
                copy.start()

    def reduce_step(i, c):
        source = acc if i == 0 else held[i - 1]
        if i < stages - 1:
            def keep(g, k, total):
                held[i][c, g, k] = total

            summed(i, source, c, keep)
            send_parts(i + 1, held[i], c)
        else:
            sums = []
            summed(i, source, c, lambda g, k, total: sums.append(total))
            gate, up = sums
            gath[(c, *mine)] = (gate / (1.0 + jnp.exp(-gate)) * up).astype(jnp.bfloat16)
            ag_start(0, c)

    def gather_step(a, c):
        ag_wait(a, c)
        if a < stages - 1:
            ag_start(a + 1, c)
        else:
            out_copy(c).start()

    steps = [multiply]
    steps += [functools.partial(reduce_step, i) for i in range(stages)]
    steps += [functools.partial(gather_step, a) for a in range(stages)]

    def turn(t, carry):
        for s, step in enumerate(steps):
            c = t - s * LAG

            @pl.when(jnp.logical_and(c >= 0, c < chunks))
            def _(c=c, step=step):
                step(c)

        return carry

    lax.fori_loop(0, chunks + (len(steps) - 1) * LAG, turn, 0)

    def drain(c, carry):
        for i in range(stages):
            for o in range(1, digits[i][1]):
                rs_copy(i, o, c).wait_send()
        for a in range(stages):
            for o in range(1, digits[order[a]][1]):
                ag_copy(a, o, c, 0).wait_send()
        out_copy(c).wait()
        return carry

    lax.fori_loop(0, chunks, drain, 0)


def solution(mesh):
    n_row, n_col = mesh.shape["row"], mesh.shape["col"]

    def local(tokens, gate_weight, up_weight):
        own_tokens, depth = tokens.shape
        columns = gate_weight.shape[1]
        each = own_tokens * n_row // n_col
        width = max(w for w in range(128, WIDEST + 1, 128) if columns % w == 0)
        chunks = columns // width
        digits = digits_of(n_col)
        radices = tuple(radix for _, radix in digits)
        subs, count = [], n_col
        for radix in radices:
            count //= radix
            subs.append(count)
        parts = [(chunks, radix - 1, 2, each, sub * width + LANES) for radix, sub in zip(radices, subs)]
        scratch = [
            pltpu.VMEM((n_row, own_tokens, depth), jnp.bfloat16),
            pltpu.VMEM((BUFFERS, 2, depth, width), jnp.bfloat16),
            pltpu.VMEM((chunks, n_col, 2, each, width), jnp.float32),
        ]
        scratch += [pltpu.VMEM((chunks, sub, 2, each, width), jnp.float32) for sub in subs[:-1]]
        scratch += [pltpu.VMEM(shape, jnp.bfloat16) for shape in parts]
        scratch += [pltpu.VMEM(shape, jnp.bfloat16) for shape in parts]
        scratch += [pltpu.VMEM((chunks, *radices, each, width), jnp.bfloat16)]
        dma = pltpu.SemaphoreType.DMA
        scratch += [dma, dma((n_row - 1,)), dma((n_row - 1,)), dma((BUFFERS, 2)), dma((chunks,))]
        for _ in range(2):
            scratch += [dma((radix - 1, chunks)) for radix in radices]
        ordered = radices[::-1] if GATHER_REVERSED else radices
        for _ in range(2):
            scratch += [dma((radix - 1, chunks)) for radix in ordered]
        out = pl.pallas_call(
            functools.partial(kernel, n_row, n_col, chunks, width),
            out_shape=jax.ShapeDtypeStruct((*radices, each, columns), jnp.bfloat16),
            in_specs=[pl.BlockSpec(memory_space=pl.ANY)] * 3,
            out_specs=pl.BlockSpec(memory_space=pl.ANY),
            scratch_shapes=scratch,
            compiler_params=pltpu.CompilerParams(
                collective_id=0, has_side_effects=True, vmem_limit_bytes=60 * 2**20),
        )(tokens, gate_weight, up_weight)
        return out.reshape(n_col * each, columns)

    in_specs = (P("row", "col"), P("col", "row"), P("col", "row"))
    return jax.shard_map(local, mesh=mesh, in_specs=in_specs, out_specs=P(None, "row"), check_vma=False)
```
